32 devices in a mesh: ka: 8 (over y, x, core), ga: 4 (over z).
Axes of the slice: x: 2, y: 2, z: 4, core: 2. Of those that a mesh axis runs over, the one named last changes fastest.
Arguments:
- psi: bfloat16 [8, 2, 128, 1024], P('ka', None, None, 'ga'), may hold values from -0.75 to 0.75
- dvscf: bfloat16 [96, 2, 1024], P(None, None, 'ga'), may hold values from -6 to 6
- kq_map: int32 [8], P('ka'), may hold values from 0 to 7, each once
Outputs:
- coupling: float32 [96, 8, 2, 128, 128], P('ga', 'ka')
The draws below stay inside these ranges and needn't reach their ends.
Inputs may be any that keep to these rules, and one draw needn't show every extreme that they name: kq_map is a permutation of the k-points 0 to 7.
All inputs are finite; a program needn't handle non-finite values.
Results may differ from the reference program's by a relative error of at most 0.0029.
Values may be sent and summed in bfloat16 or wider, within the bound.
A program may use at most 128 MiB of HBM per device.

```python
import jax
import jax.numpy as jnp
from jax import lax

BANDS = 128
MODES = 96
KPTS = 8
CELLS = 1024


def block_scale(stream_key, shape, cuts, least, high):
    loudness = 1.0
    for dim, parts in cuts:
        steps = jax.random.uniform(jax.random.fold_in(jax.random.fold_in(stream_key, 6), dim), (parts,), jnp.float32, least / len(cuts), high / len(cuts))
        loudness = loudness * jnp.repeat(jnp.exp(steps), shape[dim] // parts).reshape((-1,) + (1,) * (len(shape) - 1 - dim))
    return loudness


def noise(stream_key, shape, width, reach, cuts=(), dtype=jnp.bfloat16):
    values = width * jax.random.normal(stream_key, shape, jnp.float32)
    if cuts:
        values = values * block_scale(stream_key, shape, cuts, -0.22, 0.18)
    return jnp.clip(values, -reach, reach).astype(dtype)


def setup_inputs(seed: int = 0) -> dict:
    key_list = jax.random.split(jax.random.key(seed), 4)
    return {
        "psi": noise(key_list[0], (KPTS, 2, BANDS, CELLS), ((4 * CELLS) ** -0.25), 0.75, ((0, 8), (3, 4))),
        "dvscf": noise(key_list[1], (MODES, 2, CELLS), 1.0, 6.0, ((2, 4),)),
        "kq_map": jax.random.permutation(key_list[2], KPTS).astype(jnp.int32),
    }


def reference(psi, dvscf, kq_map):
    phi_all = jnp.take(psi, kq_map.astype(jnp.int32), axis=0)
    dv_real = dvscf[:, 0].astype(jnp.float32)[:, None, :]
    dv_imag = dvscf[:, 1].astype(jnp.float32)[:, None, :]

    def per_point(pair):
        wave, other = pair
        wave_real = wave[0].astype(jnp.float32)[None]
        wave_imag = wave[1].astype(jnp.float32)[None]
        prod_real = (dv_real * wave_real - dv_imag * wave_imag).astype(jnp.bfloat16)
        prod_imag = (dv_real * wave_imag + dv_imag * wave_real).astype(jnp.bfloat16)
        left = jnp.concatenate([other[0], other[1]], axis=-1).astype(jnp.float32)
        right_real = jnp.concatenate([prod_real, prod_imag], axis=-1).astype(jnp.float32)
        right_imag = jnp.concatenate([prod_imag, -prod_real], axis=-1).astype(jnp.float32)
        part_real = jnp.einsum('mr,unr->umn', left, right_real)
        part_imag = jnp.einsum('mr,unr->umn', left, right_imag)
        return jnp.stack([part_real, part_imag], axis=1)

    result = lax.map(per_point, (psi, phi_all))
    return jnp.transpose(result, (1, 0, 2, 3, 4))
```

```python
import functools

import jax
import jax.numpy as jnp
from jax import lax
from jax.experimental import pallas as pl
from jax.experimental.pallas import tpu as pltpu
from jax.sharding import PartitionSpec as P

MESH = pl.DeviceIdType.MESH
BLOCK = 8


def slab_at(ga, gn, step):
    return ga ^ step if gn & (gn - 1) == 0 else lax.rem(ga + step, gn)


def pairs_of(gn):
    halves = [(0, 0), (0, 1)] + [(s, 1) for s in range(1, gn)] + [(s, 0) for s in range(1, gn)]
    return [halves[2 * c:2 * c + 2] for c in range(gn)]


def exchange(
    kn, gn, psi_hbm, dv_hbm, kq_ref, partial, tail_prods, phi_near,
    dv_ref, psi_near, psi_wide, phi_wide, dv_all, dv_f32, kq_all,
    stage_near, stage_wide, choice_near, choice_wide, prods,
    load, send_kq, send_one, send_own, send_slab, send_dv, send_psi, send_phi, send_stage,
    recv_kq, recv_one, recv_own, recv_slab, recv_dv, recv_psi, recv_phi, recv_stage,
):
    ka = lax.axis_index("ka")
    ga = lax.axis_index("ga")
    rows, half = stage_near.shape[1], stage_near.shape[2]
    bands = kn * rows // 2
    modes = partial.shape[0]
    others = pl.ds(0, kn - 1)

    def along_k(d):
        return lax.rem(ka + d, kn)

    def along_g(d):
        return lax.rem(ga + d, gn)

    first_half, second_half = pl.ds(0, half), pl.ds(half, half)
    loads = [
        pltpu.make_async_copy(psi_hbm.at[:, :, second_half], psi_wide.at[ga], load.at[0]),
        pltpu.make_async_copy(psi_hbm.at[:, :, first_half], psi_near.at[ga], load.at[1]),
        pltpu.make_async_copy(psi_hbm.at[ka, :, first_half], stage_near.at[ka], load.at[2]),
        pltpu.make_async_copy(psi_hbm.at[ka, :, second_half], stage_wide.at[ga, ka], load.at[3]),
        pltpu.make_async_copy(dv_hbm, dv_ref, load.at[4]),
    ]
    for c in loads:
        c.start()
    barrier = pltpu.get_barrier_semaphore()
    for d in range(1, gn):
        pl.semaphore_signal(barrier, inc=1, device_id=(ka, along_g(d)), device_id_type=MESH)
    for d in range(1, kn):
        pl.semaphore_signal(barrier, inc=1, device_id=(along_k(d), ga), device_id_type=MESH)
    for c in loads:
        c.wait()
    dv_all[ga] = dv_ref[ga]
    kq_all[ka] = kq_ref[...]
    pl.semaphore_wait(barrier, kn + gn - 2)

    def copy(src, dst, send, recv, to):
        return pltpu.make_async_remote_copy(
            src_ref=src, dst_ref=dst, send_sem=send, recv_sem=recv, device_id=to, device_id_type=MESH
        )

    def await_recv(ref, sem):
        copy(ref, ref, load.at[0], sem, (ka, ga)).wait_recv()

    def await_send(ref, sem):
        copy(ref, ref, sem, load.at[0], (ka, ga)).wait_send()

    def kq_start(d):
        copy(kq_ref, kq_all.at[ka], send_kq.at[0], recv_kq.at[0], (along_k(d), ga)).start()

    def one_start(side, d):
        to = along_k(d)
        if side:
            copy(psi_wide.at[ga, to], stage_wide.at[ga, ka], send_one.at[1], recv_one.at[1], (to, ga)).start()
        else:
            copy(psi_near.at[ga, to], stage_near.at[ka], send_one.at[0], recv_one.at[0], (to, ga)).start()

    def own_start(side, d):
        to = along_k(d)
        if side:
            copy(choice_wide.at[ga, to], phi_wide.at[ga, ka], send_own.at[1], recv_own.at[1], (to, ga)).start()
        else:
            copy(choice_near.at[to], phi_near.at[ga, ka], send_own.at[0], recv_own.at[0], (to, ga)).start()

    def slab_start(slab, d):
        to = along_k(d)
        copy(stage_wide.at[slab, to], psi_wide.at[slab, ka], send_slab.at[0], recv_slab.at[0, slab], (to, ga)).start()
        copy(choice_wide.at[slab, to], phi_wide.at[slab, ka], send_slab.at[1], recv_slab.at[1, slab], (to, ga)).start()

    def dv_start(d):
        copy(dv_ref.at[along_g(d)], dv_all.at[ga], send_dv.at[0], recv_dv.at[0], (ka, along_g(d))).start()

    def slab_copy(all_ref, send, recv, slab, to):
        return copy(all_ref.at[slab], all_ref.at[slab], send.at[to], recv.at[slab], (ka, to))

    def spread(copies):
        for hop in range(1, max(gn - 1, 2)):
            for to in (ga + hop, ga - hop):
                @pl.when((to >= 0) & (to < gn))
                def _():
                    copies(ga, to)

    def forward(copies):
        if gn > 2:
            @pl.when(ga == 1)
            def _():
                copies(gn - 1, 0)

            @pl.when(ga == gn - 2)
            def _():
                copies(0, gn - 1)

    def is_far(slab):
        if gn <= 2:
            return ga < 0
        return ((ga == 1) & (slab == gn - 1)) | ((ga == gn - 2) & (slab == 0))

    psi_slab = functools.partial(slab_copy, psi_near, send_psi, recv_psi)
    phi_slab = functools.partial(slab_copy, phi_near, send_phi, recv_phi)
    stage_slab = functools.partial(slab_copy, stage_wide, send_stage, recv_stage)

    def pass_on(slabs, far, to):
        slabs(far, ga).wait_recv()
        slabs(far, to).start()

    def await_slab(slabs, slab):
        @pl.when(jnp.logical_not(is_far(slab)))
        def _():
            slabs(slab, ga).wait_recv()

    def choose(pieces, picks):
        def step(k, _):
            wanted = jnp.broadcast_to(kq_all[k], (rows, half))
            picked = jnp.zeros((rows, half), jnp.float32)
            for j in range(kn):
                picked = jnp.where(wanted == j, pieces[j].astype(jnp.float32), picked)
            picks[k] = picked.astype(jnp.bfloat16)
            return 0

        lax.fori_loop(0, kn, step, 0)

    spots = {half_slab: (c, i) for c, pair in enumerate(pairs_of(gn)) for i, half_slab in enumerate(pair)}

    def products(place, side):
        slab = slab_at(ga, gn, place)
        waves = psi_wide if side else psi_near
        lanes = slice(side * half, (side + 1) * half)
        chunk, start = spots[place, side]
        into = slice(start * half, (start + 1) * half)
        target = tail_prods if chunk == gn - 1 else prods.at[chunk]

        def step(u, _):
            wave = waves[slab].reshape(2 * bands, half)
            wave_real = wave[:bands].astype(jnp.float32)
            wave_imag = wave[bands:].astype(jnp.float32)
            dv = dv_f32[slab, u]
            dv_real, dv_imag = dv[0:1, lanes], dv[1:2, lanes]
            target[u, :bands, into] = (dv_real * wave_real - dv_imag * wave_imag).astype(jnp.bfloat16)
            target[u, bands:, into] = (dv_real * wave_imag + dv_imag * wave_real).astype(jnp.bfloat16)
            return 0

        lax.fori_loop(0, modes, step, 0, unroll=2)

    def widen(slab):
        dv_f32[slab] = dv_all[slab].astype(jnp.float32)

    block = BLOCK if modes % BLOCK == 0 else 1

    def matmul(chunk):
        sides = [(phi_wide if side else phi_near, slab_at(ga, gn, place)) for place, side in pairs_of(gn)[chunk]]

        def mode_step(t, _):
            other = jnp.concatenate([ref[slab].reshape(2 * bands, half) for ref, slab in sides], axis=1)
            full = lax.dot_general(
                prods[chunk, pl.ds(t * block, block)].reshape(block * 2 * bands, 2 * half),
                other, (((1,), (1,)), ((), ())), preferred_element_type=jnp.float32,
            )
            for q in range(block):
                u = t * block + q
                top, low = full[2 * q * bands:(2 * q + 1) * bands], full[(2 * q + 1) * bands:(2 * q + 2) * bands]
                real = top[:, :bands] + low[:, bands:]
                imag = low[:, :bands] - top[:, bands:]
                if chunk:
                    real = real + partial[u, 0]
                    imag = imag + partial[u, 1]
                partial[u, 0] = real
                partial[u, 1] = imag
            return 0

        lax.fori_loop(0, modes // block, mode_step, 0)

    for d in range(1, kn):
        kq_start(d)
        one_start(1, d)
    for d in range(1, kn):
        one_start(0, d)
    spread(lambda slab, to: psi_slab(slab, to).start())
    widen(ga)
    products(0, 0)
    products(0, 1)
    await_recv(kq_all.at[others], recv_kq.at[0])
    await_recv(stage_wide.at[ga, others], recv_one.at[1])
    spread(lambda slab, to: stage_slab(slab, to).start())
    for d in range(1, gn):
        dv_start(d)
    await_recv(stage_near.at[others], recv_one.at[0])
    choose(stage_near, choice_near)
    for d in range(1, kn):
        own_start(0, d)
    choose(stage_wide.at[ga], choice_wide.at[ga])
    for d in range(1, kn):
        own_start(1, d)
    phi_near[ga, ka] = choice_near[ka]
    phi_wide[ga, ka] = choice_wide[ga, ka]
    forward(functools.partial(pass_on, psi_slab))
    await_recv(phi_near.at[ga, others], recv_own.at[0])
    spread(lambda slab, to: phi_slab(slab, to).start())

    forward(functools.partial(pass_on, stage_slab))
    await_recv(dv_all.at[pl.ds(0, gn - 1)], recv_dv.at[0])
    for step in range(1, gn):
        slab = slab_at(ga, gn, step)
        await_slab(stage_slab, slab)
        choose(stage_wide.at[slab], choice_wide.at[slab])
        for d in range(1, kn):
            slab_start(slab, d)
        psi_wide[slab, ka] = stage_wide[slab, ka]
        phi_wide[slab, ka] = choice_wide[slab, ka]
        widen(slab)
        await_slab(psi_slab, slab)
        products(step, 0)
    await_recv(phi_wide.at[ga, others], recv_own.at[1])
    matmul(0)
    forward(functools.partial(pass_on, phi_slab))
    for chunk in range(1, gn):
        for place, side in pairs_of(gn)[chunk]:
            slab = slab_at(ga, gn, place)
            if side:
                await_recv(psi_wide.at[slab, others], recv_slab.at[0, slab])
                await_recv(phi_wide.at[slab, others], recv_slab.at[1, slab])
                products(place, 1)
            else:
                await_slab(phi_slab, slab)
        if chunk < gn - 1:
            matmul(chunk)

    await_send(kq_all.at[others], send_kq.at[0])
    for side in range(2):
        await_send(stage_near.at[others], send_one.at[side])
        await_send(stage_near.at[others], send_own.at[side])
        await_send(stage_wide.at[pl.ds(0, gn - 1), others], send_slab.at[side])
    await_send(dv_ref.at[pl.ds(0, gn - 1)], send_dv.at[0])
    for slabs in (psi_slab, phi_slab, stage_slab):
        spread(lambda own, to, slabs=slabs: slabs(own, to).wait_send())
        forward(lambda far, to, slabs=slabs: slabs(far, to).wait_send())


def finish(gn, partial, prods, phi_near, out_hbm, out, done):
    ga = lax.axis_index("ga")
    modes, _, bands, _ = partial.shape
    half = phi_near.shape[3]
    slabs = [slab_at(ga, gn, place) for place, _ in pairs_of(gn)[gn - 1]]
    other = jnp.concatenate([phi_near[slab].reshape(2 * bands, half) for slab in slabs], axis=1)

    def mode_step(u, _):
        full = lax.dot_general(prods[u], other, (((1,), (1,)), ((), ())), preferred_element_type=jnp.float32)
        top, low = full[:bands], full[bands:]
        out[u, 0] = (partial[u, 0] + (top[:, :bands] + low[:, bands:])).T
        out[u, 1] = (partial[u, 1] + (low[:, :bands] - top[:, bands:])).T
        pltpu.make_async_copy(out.at[u], out_hbm.at[u], done).start()
        return 0

    lax.fori_loop(0, modes, mode_step, 0, unroll=24)
    pltpu.make_async_copy(out, out_hbm, done).wait()


def body(psi, dvscf, kq_map):
    kn, gn = lax.axis_size("ka"), lax.axis_size("ga")
    _, parts, bands, cells = psi.shape
    rows = parts * bands // kn
    half = cells // 2
    modes = dvscf.shape[0] // gn
    pieces = pltpu.with_memory_space_constraint(psi.reshape(kn, rows, cells), pltpu.HBM)
    potential = pltpu.with_memory_space_constraint(dvscf.reshape(gn, modes, 2, cells), pltpu.HBM)
    wanted = jnp.broadcast_to(kq_map[:, None], (1, half)).astype(jnp.int32)
    dma = pltpu.SemaphoreType.DMA
    bf16 = jnp.bfloat16
    in_hbm, in_vmem = pl.BlockSpec(memory_space=pltpu.HBM), pl.BlockSpec(memory_space=pltpu.VMEM)
    partial, prods, phi_near = pl.pallas_call(
        functools.partial(exchange, kn, gn),
        out_shape=[
            jax.ShapeDtypeStruct((modes, 2, bands, bands), jnp.float32),
            jax.ShapeDtypeStruct((modes, 2 * bands, cells), bf16),
            jax.ShapeDtypeStruct((gn, kn, rows, half), bf16),
        ],
        in_specs=[in_hbm, in_hbm, in_vmem],
        out_specs=[in_vmem] * 3,
        scratch_shapes=[
            pltpu.VMEM((gn, modes, 2, cells), bf16),
            pltpu.VMEM((gn, kn, rows, half), bf16),
            pltpu.VMEM((gn, kn, rows, half), bf16),
            pltpu.VMEM((gn, kn, rows, half), bf16),
            pltpu.VMEM((gn, modes, 2, cells), bf16),
            pltpu.VMEM((gn, modes, 2, cells), jnp.float32),
            pltpu.VMEM((kn, 1, half), jnp.int32),
            pltpu.VMEM((kn, rows, half), bf16),
            pltpu.VMEM((gn, kn, rows, half), bf16),
            pltpu.VMEM((kn, rows, half), bf16),
            pltpu.VMEM((gn, kn, rows, half), bf16),
            pltpu.VMEM((gn - 1, modes, 2 * bands, cells), bf16),
            dma((5,)),
            dma((1,)), dma((2,)), dma((2,)), dma((2,)), dma((1,)), dma((gn,)), dma((gn,)), dma((gn,)),
            dma((1,)), dma((2,)), dma((2,)), dma((2, gn)), dma((1,)), dma((gn,)), dma((gn,)), dma((gn,)),
        ],
        compiler_params=pltpu.CompilerParams(collective_id=0, has_side_effects=True, vmem_limit_bytes=40 * 1024 * 1024),
    )(pieces, potential, wanted)
    out = pl.pallas_call(
        functools.partial(finish, gn),
        out_shape=jax.ShapeDtypeStruct((modes, 2, bands, bands), jnp.float32),
        in_specs=[in_vmem] * 3,
        out_specs=in_hbm,
        scratch_shapes=[pltpu.VMEM((modes, 2, bands, bands), jnp.float32), dma],
        compiler_params=pltpu.CompilerParams(vmem_limit_bytes=16 * 1024 * 1024),
    )(partial, prods, phi_near)
    return out[:, None]


def solution(mesh):
    return jax.shard_map(
        body,
        mesh=mesh,
        in_specs=(P("ka", None, None, "ga"), P(None, None, "ga"), P("ka")),
        out_specs=P("ga", "ka", None, None, None),
        check_vma=False,
    )
```

```python
import functools

import jax
import jax.numpy as jnp
from jax import lax
from jax.experimental import pallas as pl
from jax.experimental.pallas import tpu as pltpu
from jax.sharding import PartitionSpec as P

MESH = pl.DeviceIdType.MESH
BLOCK = 8
BAND_BLOCK = 32
UNROLL = 24
PSI = (False, False)
STAGE = (False, False)
PHI = (False, False)


def slab_at(ga, gn, step):
    if step == 0:
        return ga
    below, above = ga, gn - 1 - ga
    both = jnp.minimum(below, above)
    near = ga + (step + 1) // 2 if step % 2 else ga - step // 2
    far = jnp.where(above > below, ga + (step - both), ga - (step - both))
    return jnp.where(step <= 2 * both, near, far)


def pairs_of(gn):
    halves = [(0, 0), (0, 1)] + [(s, 1) for s in range(1, gn)] + [(s, 0) for s in range(1, gn)]
    return [halves[2 * c:2 * c + 2] for c in range(gn)]


def exchange(
    kn, gn, psi_hbm, dv_hbm, kq_ref, partial, tail_prods, phi_near,
    dv_ref, psi_near, psi_wide, phi_wide, dv_all, dv_f32, kq_all,
    stage_near, stage_wide, choice_near, choice_wide, prods,
    load, send_kq, send_one, send_own, send_slab, send_dv, send_psi, send_phi, send_stage,
    recv_kq, recv_one, recv_own, recv_slab, recv_dv, recv_psi, recv_phi, recv_stage,
):
    ka = lax.axis_index("ka")
    ga = lax.axis_index("ga")
    rows, half = stage_near.shape[1], stage_near.shape[2]
    bands = kn * rows // 2
    modes = partial.shape[0]
    others = pl.ds(0, kn - 1)

    def along_k(d):
        return lax.rem(ka + d, kn)

    def along_g(d):
        return lax.rem(ga + d, gn)

    first_half, second_half = pl.ds(0, half), pl.ds(half, half)
    loads = [
        pltpu.make_async_copy(psi_hbm.at[:, :, second_half], psi_wide.at[ga], load.at[0]),
        pltpu.make_async_copy(psi_hbm.at[:, :, first_half], psi_near.at[ga], load.at[1]),
        pltpu.make_async_copy(psi_hbm.at[ka, :, first_half], stage_near.at[ka], load.at[2]),
        pltpu.make_async_copy(psi_hbm.at[ka, :, second_half], stage_wide.at[ga, ka], load.at[3]),
        pltpu.make_async_copy(dv_hbm, dv_ref, load.at[4]),
    ]
    for c in loads:
        c.start()
    barrier = pltpu.get_barrier_semaphore()
    for d in range(1, gn):
        pl.semaphore_signal(barrier, inc=1, device_id=(ka, along_g(d)), device_id_type=MESH)
    for d in range(1, kn):
        pl.semaphore_signal(barrier, inc=1, device_id=(along_k(d), ga), device_id_type=MESH)
    for c in loads:
        c.wait()
    kq_all[ka] = kq_ref[...]
    pl.semaphore_wait(barrier, kn + gn - 2)

    def copy(src, dst, send, recv, to):
        return pltpu.make_async_remote_copy(
            src_ref=src, dst_ref=dst, send_sem=send, recv_sem=recv, device_id=to, device_id_type=MESH
        )

    def await_recv(ref, sem):
        copy(ref, ref, load.at[0], sem, (ka, ga)).wait_recv()

    def await_send(ref, sem):
        copy(ref, ref, sem, load.at[0], (ka, ga)).wait_send()

    def kq_start(d):
        copy(kq_ref, kq_all.at[ka], send_kq.at[0], recv_kq.at[0], (along_k(d), ga)).start()

    def one_start(side, d):
        to = along_k(d)
        if side:
            copy(psi_wide.at[ga, to], stage_wide.at[ga, ka], send_one.at[1], recv_one.at[1], (to, ga)).start()
        else:
            copy(psi_near.at[ga, to], stage_near.at[ka], send_one.at[0], recv_one.at[0], (to, ga)).start()

    def own_start(side, d):
        to = along_k(d)
        if side:
            copy(choice_wide.at[ga, to], phi_wide.at[ga, ka], send_own.at[1], recv_own.at[1], (to, ga)).start()
        else:
            copy(choice_near.at[to], phi_near.at[ga, ka], send_own.at[0], recv_own.at[0], (to, ga)).start()

    def slab_start(slab, d):
        to = along_k(d)
        copy(stage_wide.at[slab, to], psi_wide.at[slab, ka], send_slab.at[0], recv_slab.at[0, slab], (to, ga)).start()
        copy(choice_wide.at[slab, to], phi_wide.at[slab, ka], send_slab.at[1], recv_slab.at[1, slab], (to, ga)).start()

    shares, share = dv_all.shape[0], dv_all.shape[2]
    own_share = ka if shares > 1 else 0

    def dv_start(d):
        piece = dv_ref.at[along_g(d), pl.ds(own_share * share, share)]
        copy(piece, dv_all.at[own_share, ga], send_dv.at[0], recv_dv.at[0], (ka, along_g(d))).start()

    def dv_share_start(d):
        copy(dv_all.at[ka], dv_all.at[ka], send_dv.at[1], recv_dv.at[1], (along_k(d), ga)).start()

    def slab_copy(all_ref, send, recv, slab, to):
        return copy(all_ref.at[slab], all_ref.at[slab], send.at[to], recv.at[slab], (ka, to))

    def spread(slabs, act):
        hops = range(1, gn) if slabs.direct else range(1, max(gn - 1, 2))
        for hop in reversed(hops) if slabs.far_first else hops:
            for to in (ga + hop, ga - hop):
                @pl.when((to >= 0) & (to < gn))
                def _():
                    act(slabs, ga, to)

    def forward(slabs, act):
        copies = functools.partial(act, slabs)
        if gn > 2 and not slabs.direct:
            @pl.when(ga == 1)
            def _():
                copies(gn - 1, 0)

            @pl.when(ga == gn - 2)
            def _():
                copies(0, gn - 1)

    def is_far(slab):
        if gn <= 2:
            return ga < 0
        return ((ga == 1) & (slab == gn - 1)) | ((ga == gn - 2) & (slab == 0))

    psi_slab = functools.partial(slab_copy, psi_near, send_psi, recv_psi)
    phi_slab = functools.partial(slab_copy, phi_near, send_phi, recv_phi)
    stage_slab = functools.partial(slab_copy, stage_wide, send_stage, recv_stage)
    psi_slab.direct, psi_slab.far_first = PSI
    phi_slab.direct, phi_slab.far_first = PHI
    stage_slab.direct, stage_slab.far_first = STAGE

    def start(slabs, slab, to):
        slabs(slab, to).start()

    def finish_send(slabs, slab, to):
        slabs(slab, to).wait_send()

    def pass_on(slabs, far, to):
        slabs(far, ga).wait_recv()
        slabs(far, to).start()

    def await_slab(slabs, slab):
        if slabs.direct:
            slabs(slab, ga).wait_recv()
        else:
            @pl.when(jnp.logical_not(is_far(slab)))
            def _():
                slabs(slab, ga).wait_recv()

    def choose(pieces, picks):
        def step(k, _):
            wanted = jnp.broadcast_to(kq_all[k], (rows, half))
            picked = jnp.zeros((rows, half), jnp.float32)
            for j in range(kn):
                picked = jnp.where(wanted == j, pieces[j].astype(jnp.float32), picked)
            picks[k] = picked.astype(jnp.bfloat16)
            return 0

        lax.fori_loop(0, kn, step, 0)

    spots = {half_slab: (c, i) for c, pair in enumerate(pairs_of(gn)) for i, half_slab in enumerate(pair)}

    def products(place, side):
        slab = slab_at(ga, gn, place)
        waves = psi_wide if side else psi_near
        lanes = slice(side * half, (side + 1) * half)
        chunk, start = spots[place, side]
        into = slice(start * half, (start + 1) * half)
        target = tail_prods if chunk == gn - 1 else prods.at[chunk]

        wave = waves.at[slab]
        span = min(BAND_BLOCK, rows)
        for first in range(0, bands, span):
            wave_real = wave[first // rows, first % rows:first % rows + span].astype(jnp.float32)
            low = bands + first
            wave_imag = wave[low // rows, low % rows:low % rows + span].astype(jnp.float32)

            def step(u, _):
                dv = dv_f32[slab, u]
                dv_real, dv_imag = dv[0:1, lanes], dv[1:2, lanes]
                target[u, first:first + span, into] = (dv_real * wave_real - dv_imag * wave_imag).astype(jnp.bfloat16)
                target[u, low:low + span, into] = (dv_real * wave_imag + dv_imag * wave_real).astype(jnp.bfloat16)
                return 0

            lax.fori_loop(0, modes, step, 0, unroll=UNROLL)

    def widen(slab):
        for i in range(shares):
            dv_f32[slab, i * share:(i + 1) * share] = dv_all[i, slab].astype(jnp.float32)

    block = BLOCK if modes % BLOCK == 0 else 1

    def matmul(chunk):
        sides = [(phi_wide if side else phi_near, slab_at(ga, gn, place)) for place, side in pairs_of(gn)[chunk]]

        def mode_step(t, _):
            other = jnp.concatenate([ref[slab].reshape(2 * bands, half) for ref, slab in sides], axis=1)
            full = lax.dot_general(
                prods[chunk, pl.ds(t * block, block)].reshape(block * 2 * bands, 2 * half),
                other, (((1,), (1,)), ((), ())), preferred_element_type=jnp.float32,
            )
            for q in range(block):
                u = t * block + q
                top, low = full[2 * q * bands:(2 * q + 1) * bands], full[(2 * q + 1) * bands:(2 * q + 2) * bands]
                real = top[:, :bands] + low[:, bands:]
                imag = low[:, :bands] - top[:, bands:]
                if chunk:
                    real = real + partial[u, 0]
                    imag = imag + partial[u, 1]
                partial[u, 0] = real
                partial[u, 1] = imag
            return 0

        lax.fori_loop(0, modes // block, mode_step, 0, unroll=True)

    for d in range(1, kn):
        kq_start(d)
        one_start(1, d)
    for d in range(1, gn):
        dv_start(d)
    for d in range(1, kn):
        one_start(0, d)
    spread(psi_slab, start)
    dv_f32[ga] = dv_ref[ga].astype(jnp.float32)
    products(0, 0)
    products(0, 1)
    await_recv(kq_all.at[others], recv_kq.at[0])
    await_recv(stage_wide.at[ga, others], recv_one.at[1])
    spread(stage_slab, start)
    await_recv(stage_near.at[others], recv_one.at[0])
    choose(stage_near, choice_near)
    for d in range(1, kn):
        own_start(0, d)
    await_recv(dv_all.at[0, pl.ds(0, gn - 1)], recv_dv.at[0])
    if shares > 1:
        for d in range(1, kn):
            dv_share_start(d)
    choose(stage_wide.at[ga], choice_wide.at[ga])
    for d in range(1, kn):
        own_start(1, d)
    phi_near[ga, ka] = choice_near[ka]
    phi_wide[ga, ka] = choice_wide[ga, ka]
    forward(psi_slab, pass_on)
    await_recv(phi_near.at[ga, others], recv_own.at[0])
    spread(phi_slab, start)
    if shares > 1:
        await_recv(dv_all.at[others], recv_dv.at[1])

    def relay_step(step):
        slab = slab_at(ga, gn, step)
        await_slab(stage_slab, slab)
        choose(stage_wide.at[slab], choice_wide.at[slab])
        for d in range(1, kn):
            slab_start(slab, d)
        psi_wide[slab, ka] = stage_wide[slab, ka]
        phi_wide[slab, ka] = choice_wide[slab, ka]

    def near_step(step):
        slab = slab_at(ga, gn, step)
        widen(slab)
        await_slab(psi_slab, slab)
        products(step, 0)

    forward(stage_slab, pass_on)
    for step in range(1, gn):
        relay_step(step)
        near_step(step)
    await_recv(phi_wide.at[ga, others], recv_own.at[1])
    matmul(0)
    forward(phi_slab, pass_on)
    for chunk in range(1, gn):
        for place, side in pairs_of(gn)[chunk]:
            slab = slab_at(ga, gn, place)
            if side:
                await_recv(psi_wide.at[slab, others], recv_slab.at[0, slab])
                await_recv(phi_wide.at[slab, others], recv_slab.at[1, slab])
                products(place, 1)
            else:
                await_slab(phi_slab, slab)
        if chunk < gn - 1:
            matmul(chunk)

    await_send(kq_all.at[others], send_kq.at[0])
    for side in range(2):
        await_send(stage_near.at[others], send_one.at[side])
        await_send(stage_near.at[others], send_own.at[side])
        await_send(stage_wide.at[pl.ds(0, gn - 1), others], send_slab.at[side])
    await_send(dv_all.at[0, pl.ds(0, gn - 1)], send_dv.at[0])
    if shares > 1:
        await_send(dv_all.at[others], send_dv.at[1])
    for slabs in (psi_slab, phi_slab, stage_slab):
        spread(slabs, finish_send)
        forward(slabs, finish_send)


def finish(gn, partial, prods, phi_near, out_hbm, out, done):
    ga = lax.axis_index("ga")
    modes, _, bands, _ = partial.shape
    half = phi_near.shape[3]
    slabs = [slab_at(ga, gn, place) for place, _ in pairs_of(gn)[gn - 1]]
    other = jnp.concatenate([phi_near[slab].reshape(2 * bands, half) for slab in slabs], axis=1)

    def mode_step(u, _):
        full = lax.dot_general(prods[u], other, (((1,), (1,)), ((), ())), preferred_element_type=jnp.float32)
        top, low = full[:bands], full[bands:]
        out[u, 0] = (partial[u, 0] + (top[:, :bands] + low[:, bands:])).T
        out[u, 1] = (partial[u, 1] + (low[:, :bands] - top[:, bands:])).T
        pltpu.make_async_copy(out.at[u], out_hbm.at[u], done).start()
        return 0

    lax.fori_loop(0, modes, mode_step, 0, unroll=24)
    pltpu.make_async_copy(out, out_hbm, done).wait()


def body(psi, dvscf, kq_map):
    kn, gn = lax.axis_size("ka"), lax.axis_size("ga")
    _, parts, bands, cells = psi.shape
    rows = parts * bands // kn
    half = cells // 2
    modes = dvscf.shape[0] // gn
    shares = kn if modes % kn == 0 else 1
    pieces = pltpu.with_memory_space_constraint(psi.reshape(kn, rows, cells), pltpu.HBM)
    potential = pltpu.with_memory_space_constraint(dvscf.reshape(gn, modes, 2, cells), pltpu.HBM)
    wanted = jnp.broadcast_to(kq_map[:, None], (1, half)).astype(jnp.int32)
    dma = pltpu.SemaphoreType.DMA
    bf16 = jnp.bfloat16
    in_hbm, in_vmem = pl.BlockSpec(memory_space=pltpu.HBM), pl.BlockSpec(memory_space=pltpu.VMEM)
    partial, prods, phi_near = pl.pallas_call(
        functools.partial(exchange, kn, gn),
        out_shape=[
            jax.ShapeDtypeStruct((modes, 2, bands, bands), jnp.float32),
            jax.ShapeDtypeStruct((modes, 2 * bands, cells), bf16),
            jax.ShapeDtypeStruct((gn, kn, rows, half), bf16),
        ],
        in_specs=[in_hbm, in_hbm, in_vmem],
        out_specs=[in_vmem] * 3,
        scratch_shapes=[
            pltpu.VMEM((gn, modes, 2, cells), bf16),
            pltpu.VMEM((gn, kn, rows, half), bf16),
            pltpu.VMEM((gn, kn, rows, half), bf16),
            pltpu.VMEM((gn, kn, rows, half), bf16),
            pltpu.VMEM((shares, gn, modes // shares, 2, cells), bf16),
            pltpu.VMEM((gn, modes, 2, cells), jnp.float32),
            pltpu.VMEM((kn, 1, half), jnp.int32),
            pltpu.VMEM((kn, rows, half), bf16),
            pltpu.VMEM((gn, kn, rows, half), bf16),
            pltpu.VMEM((kn, rows, half), bf16),
            pltpu.VMEM((gn, kn, rows, half), bf16),
            pltpu.VMEM((gn - 1, modes, 2 * bands, cells), bf16),
            dma((5,)),
            dma((1,)), dma((2,)), dma((2,)), dma((2,)), dma((2,)), dma((gn,)), dma((gn,)), dma((gn,)),
            dma((1,)), dma((2,)), dma((2,)), dma((2, gn)), dma((2,)), dma((gn,)), dma((gn,)), dma((gn,)),
        ],
        compiler_params=pltpu.CompilerParams(collective_id=0, has_side_effects=True, vmem_limit_bytes=40 * 1024 * 1024),
    )(pieces, potential, wanted)
    out = pl.pallas_call(
        functools.partial(finish, gn),
        out_shape=jax.ShapeDtypeStruct((modes, 2, bands, bands), jnp.float32),
        in_specs=[in_vmem] * 3,
        out_specs=in_hbm,
        scratch_shapes=[pltpu.VMEM((modes, 2, bands, bands), jnp.float32), dma],
        compiler_params=pltpu.CompilerParams(vmem_limit_bytes=16 * 1024 * 1024),
    )(partial, prods, phi_near)
    return out[:, None]


def solution(mesh):
    return jax.shard_map(
        body,
        mesh=mesh,
        in_specs=(P("ka", None, None, "ga"), P(None, None, "ga"), P("ka")),
        out_specs=P("ga", "ka", None, None, None),
        check_vma=False,
    )
```

```python
import functools

import jax
import jax.numpy as jnp
from jax import lax
from jax.experimental import pallas as pl
from jax.experimental.pallas import tpu as pltpu
from jax.sharding import PartitionSpec as P

MESH = pl.DeviceIdType.MESH
BLOCK = 8
BAND_BLOCK = 32
UNROLL = 24
PSI = (False, False)
STAGE = (False, False)
PHI = (False, False)


def slab_at(ga, gn, step):
    if step == 0:
        return ga
    below, above = ga, gn - 1 - ga
    both = jnp.minimum(below, above)
    near = ga + (step + 1) // 2 if step % 2 else ga - step // 2
    far = jnp.where(above > below, ga + (step - both), ga - (step - both))
    return jnp.where(step <= 2 * both, near, far)


def pairs_of(gn):
    halves = [(0, 0), (0, 1)] + [(s, 1) for s in range(1, gn)] + [(s, 0) for s in range(1, gn)]
    return [halves[2 * c:2 * c + 2] for c in range(gn)]


def exchange(
    kn, gn, psi_hbm, dv_hbm, kq_ref, partial, tail_prods, phi_near,
    dv_ref, psi_near, psi_wide, phi_wide, dv_all, dv_f32, kq_all,
    stage_near, stage_wide, choice_near, choice_wide, prods,
    load, send_kq, send_one, send_own, send_slab, send_dv, send_psi, send_phi, send_stage,
    recv_kq, recv_one, recv_own, recv_slab, recv_dv, recv_psi, recv_phi, recv_stage,
):
    ka = lax.axis_index("ka")
    ga = lax.axis_index("ga")
    rows, half = stage_near.shape[1], stage_near.shape[2]
    bands = kn * rows // 2
    modes = partial.shape[0]
    others = pl.ds(0, kn - 1)

    def along_k(d):
        return lax.rem(ka + d, kn)

    def along_g(d):
        return lax.rem(ga + d, gn)

    first_half, second_half = pl.ds(0, half), pl.ds(half, half)
    loads = [
        pltpu.make_async_copy(psi_hbm.at[:, :, second_half], psi_wide.at[ga], load.at[0]),
        pltpu.make_async_copy(psi_hbm.at[:, :, first_half], psi_near.at[ga], load.at[1]),
        pltpu.make_async_copy(psi_hbm.at[ka, :, first_half], stage_near.at[ka], load.at[2]),
        pltpu.make_async_copy(psi_hbm.at[ka, :, second_half], stage_wide.at[ga, ka], load.at[3]),
        pltpu.make_async_copy(dv_hbm, dv_ref, load.at[4]),
    ]
    for c in loads:
        c.start()
    barrier = pltpu.get_barrier_semaphore()
    for d in range(1, gn):
        pl.semaphore_signal(barrier, inc=1, device_id=(ka, along_g(d)), device_id_type=MESH)
    for d in range(1, kn):
        pl.semaphore_signal(barrier, inc=1, device_id=(along_k(d), ga), device_id_type=MESH)
    for c in loads:
        c.wait()
    kq_all[ka] = kq_ref[...]
    pl.semaphore_wait(barrier, kn + gn - 2)

    def copy(src, dst, send, recv, to):
        return pltpu.make_async_remote_copy(
            src_ref=src, dst_ref=dst, send_sem=send, recv_sem=recv, device_id=to, device_id_type=MESH
        )

    def await_recv(ref, sem):
        copy(ref, ref, load.at[0], sem, (ka, ga)).wait_recv()

    def await_send(ref, sem):
        copy(ref, ref, sem, load.at[0], (ka, ga)).wait_send()

    def kq_start(d):
        copy(kq_ref, kq_all.at[ka], send_kq.at[0], recv_kq.at[0], (along_k(d), ga)).start()

    def one_start(side, d):
        to = along_k(d)
        if side:
            copy(psi_wide.at[ga, to], stage_wide.at[ga, ka], send_one.at[1], recv_one.at[1], (to, ga)).start()
        else:
            copy(psi_near.at[ga, to], stage_near.at[ka], send_one.at[0], recv_one.at[0], (to, ga)).start()

    def own_start(side, d):
        to = along_k(d)
        if side:
            copy(choice_wide.at[ga, to], phi_wide.at[ga, ka], send_own.at[1], recv_own.at[1], (to, ga)).start()
        else:
            copy(choice_near.at[to], phi_near.at[ga, ka], send_own.at[0], recv_own.at[0], (to, ga)).start()

    def slab_start(slab, d):
        to = along_k(d)
        copy(stage_wide.at[slab, to], psi_wide.at[slab, ka], send_slab.at[0], recv_slab.at[0, slab], (to, ga)).start()
        copy(choice_wide.at[slab, to], phi_wide.at[slab, ka], send_slab.at[1], recv_slab.at[1, slab], (to, ga)).start()

    shares, share = dv_all.shape[0], dv_all.shape[2]
    own_share = ka if shares > 1 else 0

    def dv_start(d):
        piece = dv_ref.at[along_g(d), pl.ds(own_share * share, share)]
        copy(piece, dv_all.at[own_share, ga], send_dv.at[0], recv_dv.at[0], (ka, along_g(d))).start()

    def dv_share_start(d):
        copy(dv_all.at[ka], dv_all.at[ka], send_dv.at[1], recv_dv.at[1], (along_k(d), ga)).start()

    def slab_copy(all_ref, send, recv, slab, to):
        return copy(all_ref.at[slab], all_ref.at[slab], send.at[to], recv.at[slab], (ka, to))

    def spread(slabs, act):
        hops = range(1, gn) if slabs.direct else range(1, max(gn - 1, 2))
        for hop in reversed(hops) if slabs.far_first else hops:
            for to in (ga + hop, ga - hop):
                @pl.when((to >= 0) & (to < gn))
                def _():
                    act(slabs, ga, to)

    def forward(slabs, act):
        copies = functools.partial(act, slabs)
        if gn > 2 and not slabs.direct:
            @pl.when(ga == 1)
            def _():
                copies(gn - 1, 0)

            @pl.when(ga == gn - 2)
            def _():
                copies(0, gn - 1)

    def is_far(slab):
        if gn <= 2:
            return ga < 0
        return ((ga == 1) & (slab == gn - 1)) | ((ga == gn - 2) & (slab == 0))

    psi_slab = functools.partial(slab_copy, psi_near, send_psi, recv_psi)
    phi_slab = functools.partial(slab_copy, phi_near, send_phi, recv_phi)
    stage_slab = functools.partial(slab_copy, stage_wide, send_stage, recv_stage)
    psi_slab.direct, psi_slab.far_first = PSI
    phi_slab.direct, phi_slab.far_first = PHI
    stage_slab.direct, stage_slab.far_first = STAGE

    def start(slabs, slab, to):
        slabs(slab, to).start()

    def finish_send(slabs, slab, to):
        slabs(slab, to).wait_send()

    def pass_on(slabs, far, to):
        slabs(far, ga).wait_recv()
        slabs(far, to).start()

    def await_slab(slabs, slab):
        if slabs.direct:
            slabs(slab, ga).wait_recv()
        else:
            @pl.when(jnp.logical_not(is_far(slab)))
            def _():
                slabs(slab, ga).wait_recv()

    def choose(pieces, picks):
        def step(k, _):
            wanted = jnp.broadcast_to(kq_all[k], (rows, half))
            picked = jnp.zeros((rows, half), jnp.float32)
            for j in range(kn):
                picked = jnp.where(wanted == j, pieces[j].astype(jnp.float32), picked)
            picks[k] = picked.astype(jnp.bfloat16)
            return 0

        lax.fori_loop(0, kn, step, 0)

    spots = {half_slab: (c, i) for c, pair in enumerate(pairs_of(gn)) for i, half_slab in enumerate(pair)}

    def products(place, side):
        slab = slab_at(ga, gn, place)
        waves = psi_wide if side else psi_near
        lanes = slice(side * half, (side + 1) * half)
        chunk, start = spots[place, side]
        into = slice(start * half, (start + 1) * half)
        target = tail_prods if chunk == gn - 1 else prods.at[chunk]

        wave = waves.at[slab]
        span = min(BAND_BLOCK, rows)
        for first in range(0, bands, span):
            wave_real = wave[first // rows, first % rows:first % rows + span].astype(jnp.float32)
            low = bands + first
            wave_imag = wave[low // rows, low % rows:low % rows + span].astype(jnp.float32)

            def step(u, _):
                dv = dv_f32[slab, u]
                dv_real, dv_imag = dv[0:1, lanes], dv[1:2, lanes]
                target[u, first:first + span, into] = (dv_real * wave_real - dv_imag * wave_imag).astype(jnp.bfloat16)
                target[u, low:low + span, into] = (dv_real * wave_imag + dv_imag * wave_real).astype(jnp.bfloat16)
                return 0

            lax.fori_loop(0, modes, step, 0, unroll=UNROLL)

    def widen(slab):
        for i in range(shares):
            dv_f32[slab, i * share:(i + 1) * share] = dv_all[i, slab].astype(jnp.float32)

    block = BLOCK if modes % BLOCK == 0 else 1

    def block_products(place, side, first_mode):
        slab = slab_at(ga, gn, place)
        wave = (psi_wide if side else psi_near).at[slab]
        lanes = slice(side * half, (side + 1) * half)
        chunk, start = spots[place, side]
        into = slice(start * half, (start + 1) * half)
        span = min(BAND_BLOCK, rows)
        for first in range(0, bands, span):
            low = bands + first
            wave_real = wave[first // rows, first % rows:first % rows + span].astype(jnp.float32)
            wave_imag = wave[low // rows, low % rows:low % rows + span].astype(jnp.float32)
            for q in range(block):
                dv = dv_f32[slab, first_mode + q]
                dv_real, dv_imag = dv[0:1, lanes], dv[1:2, lanes]
                u = first_mode + q
                real = (dv_real * wave_real - dv_imag * wave_imag).astype(jnp.bfloat16)
                imag = (dv_real * wave_imag + dv_imag * wave_real).astype(jnp.bfloat16)
                prods[chunk, u, first:first + span, into] = real
                prods[chunk, u, low:low + span, into] = imag

    def matmul(chunk, fresh=()):
        sides = [(phi_wide if side else phi_near, slab_at(ga, gn, place)) for place, side in pairs_of(gn)[chunk]]

        def mode_step(t, _):
            for place, side in fresh:
                block_products(place, side, t * block)
            other = jnp.concatenate([ref[slab].reshape(2 * bands, half) for ref, slab in sides], axis=1)
            full = lax.dot_general(
                prods[chunk, pl.ds(t * block, block)].reshape(block * 2 * bands, 2 * half),
                other, (((1,), (1,)), ((), ())), preferred_element_type=jnp.float32,
            )
            for q in range(block):
                u = t * block + q
                top, low = full[2 * q * bands:(2 * q + 1) * bands], full[(2 * q + 1) * bands:(2 * q + 2) * bands]
                real = top[:, :bands] + low[:, bands:]
                imag = low[:, :bands] - top[:, bands:]
                if chunk:
                    real = real + partial[u, 0]
                    imag = imag + partial[u, 1]
                partial[u, 0] = real
                partial[u, 1] = imag
            return 0

        lax.fori_loop(0, modes // block, mode_step, 0, unroll=True)

    for d in range(1, kn):
        kq_start(d)
        one_start(1, d)
    for d in range(1, gn):
        dv_start(d)
    for d in range(1, kn):
        one_start(0, d)
    spread(psi_slab, start)
    dv_f32[ga] = dv_ref[ga].astype(jnp.float32)
    products(0, 0)
    products(0, 1)
    await_recv(kq_all.at[others], recv_kq.at[0])
    await_recv(stage_wide.at[ga, others], recv_one.at[1])
    spread(stage_slab, start)
    await_recv(stage_near.at[others], recv_one.at[0])
    choose(stage_near, choice_near)
    for d in range(1, kn):
        own_start(0, d)
    await_recv(dv_all.at[0, pl.ds(0, gn - 1)], recv_dv.at[0])
    if shares > 1:
        for d in range(1, kn):
            dv_share_start(d)
    choose(stage_wide.at[ga], choice_wide.at[ga])
    for d in range(1, kn):
        own_start(1, d)
    phi_near[ga, ka] = choice_near[ka]
    phi_wide[ga, ka] = choice_wide[ga, ka]
    forward(psi_slab, pass_on)
    await_recv(phi_near.at[ga, others], recv_own.at[0])
    spread(phi_slab, start)
    if shares > 1:
        await_recv(dv_all.at[others], recv_dv.at[1])

    def relay_step(step):
        slab = slab_at(ga, gn, step)
        await_slab(stage_slab, slab)
        choose(stage_wide.at[slab], choice_wide.at[slab])
        for d in range(1, kn):
            slab_start(slab, d)
        psi_wide[slab, ka] = stage_wide[slab, ka]
        phi_wide[slab, ka] = choice_wide[slab, ka]

    def near_step(step):
        slab = slab_at(ga, gn, step)
        widen(slab)
        await_slab(psi_slab, slab)
        products(step, 0)

    forward(stage_slab, pass_on)
    await_recv(phi_wide.at[ga, others], recv_own.at[1])
    for step in range(1, gn):
        relay_step(step)
        if step == 1:
            matmul(0)
        if step == gn - 2:
            near_step(1)
    forward(phi_slab, pass_on)
    for step in range(2, gn):
        near_step(step)
    for chunk in range(1, gn):
        for place, side in pairs_of(gn)[chunk]:
            slab = slab_at(ga, gn, place)
            if side:
                await_recv(psi_wide.at[slab, others], recv_slab.at[0, slab])
                await_recv(phi_wide.at[slab, others], recv_slab.at[1, slab])
                if chunk == gn - 1:
                    products(place, 1)
            else:
                await_slab(phi_slab, slab)
        if chunk < gn - 1:
            matmul(chunk, [(place, side) for place, side in pairs_of(gn)[chunk] if side])

    await_send(kq_all.at[others], send_kq.at[0])
    for side in range(2):
        await_send(stage_near.at[others], send_one.at[side])
        await_send(stage_near.at[others], send_own.at[side])
        await_send(stage_wide.at[pl.ds(0, gn - 1), others], send_slab.at[side])
    await_send(dv_all.at[0, pl.ds(0, gn - 1)], send_dv.at[0])
    if shares > 1:
        await_send(dv_all.at[others], send_dv.at[1])
    for slabs in (psi_slab, phi_slab, stage_slab):
        spread(slabs, finish_send)
        forward(slabs, finish_send)


def finish(gn, partial, prods, phi_near, out_hbm, out, done):
    ga = lax.axis_index("ga")
    modes, _, bands, _ = partial.shape
    half = phi_near.shape[3]
    slabs = [slab_at(ga, gn, place) for place, _ in pairs_of(gn)[gn - 1]]
    other = jnp.concatenate([phi_near[slab].reshape(2 * bands, half) for slab in slabs], axis=1)

    def mode_step(u, _):
        full = lax.dot_general(prods[u], other, (((1,), (1,)), ((), ())), preferred_element_type=jnp.float32)
        top, low = full[:bands], full[bands:]
        out[u, 0] = (partial[u, 0] + (top[:, :bands] + low[:, bands:])).T
        out[u, 1] = (partial[u, 1] + (low[:, :bands] - top[:, bands:])).T
        pltpu.make_async_copy(out.at[u], out_hbm.at[u], done).start()
        return 0

    lax.fori_loop(0, modes, mode_step, 0, unroll=24)
    pltpu.make_async_copy(out, out_hbm, done).wait()


def body(psi, dvscf, kq_map):
    kn, gn = lax.axis_size("ka"), lax.axis_size("ga")
    _, parts, bands, cells = psi.shape
    rows = parts * bands // kn
    half = cells // 2
    modes = dvscf.shape[0] // gn
    shares = kn if modes % kn == 0 else 1
    pieces = pltpu.with_memory_space_constraint(psi.reshape(kn, rows, cells), pltpu.HBM)
    potential = pltpu.with_memory_space_constraint(dvscf.reshape(gn, modes, 2, cells), pltpu.HBM)
    wanted = jnp.broadcast_to(kq_map[:, None], (1, half)).astype(jnp.int32)
    dma = pltpu.SemaphoreType.DMA
    bf16 = jnp.bfloat16
    in_hbm, in_vmem = pl.BlockSpec(memory_space=pltpu.HBM), pl.BlockSpec(memory_space=pltpu.VMEM)
    partial, prods, phi_near = pl.pallas_call(
        functools.partial(exchange, kn, gn),
        out_shape=[
            jax.ShapeDtypeStruct((modes, 2, bands, bands), jnp.float32),
            jax.ShapeDtypeStruct((modes, 2 * bands, cells), bf16),
            jax.ShapeDtypeStruct((gn, kn, rows, half), bf16),
        ],
        in_specs=[in_hbm, in_hbm, in_vmem],
        out_specs=[in_vmem] * 3,
        scratch_shapes=[
            pltpu.VMEM((gn, modes, 2, cells), bf16),
            pltpu.VMEM((gn, kn, rows, half), bf16),
            pltpu.VMEM((gn, kn, rows, half), bf16),
            pltpu.VMEM((gn, kn, rows, half), bf16),
            pltpu.VMEM((shares, gn, modes // shares, 2, cells), bf16),
            pltpu.VMEM((gn, modes, 2, cells), jnp.float32),
            pltpu.VMEM((kn, 1, half), jnp.int32),
            pltpu.VMEM((kn, rows, half), bf16),
            pltpu.VMEM((gn, kn, rows, half), bf16),
            pltpu.VMEM((kn, rows, half), bf16),
            pltpu.VMEM((gn, kn, rows, half), bf16),
            pltpu.VMEM((gn - 1, modes, 2 * bands, cells), bf16),
            dma((5,)),
            dma((1,)), dma((2,)), dma((2,)), dma((2,)), dma((2,)), dma((gn,)), dma((gn,)), dma((gn,)),
            dma((1,)), dma((2,)), dma((2,)), dma((2, gn)), dma((2,)), dma((gn,)), dma((gn,)), dma((gn,)),
        ],
        compiler_params=pltpu.CompilerParams(collective_id=0, has_side_effects=True, vmem_limit_bytes=40 * 1024 * 1024),
    )(pieces, potential, wanted)
    out = pl.pallas_call(
        functools.partial(finish, gn),
        out_shape=jax.ShapeDtypeStruct((modes, 2, bands, bands), jnp.float32),
        in_specs=[in_vmem] * 3,
        out_specs=in_hbm,
        scratch_shapes=[pltpu.VMEM((modes, 2, bands, bands), jnp.float32), dma],
        compiler_params=pltpu.CompilerParams(vmem_limit_bytes=16 * 1024 * 1024),
    )(partial, prods, phi_near)
    return out[:, None]


def solution(mesh):
    return jax.shard_map(
        body,
        mesh=mesh,
        in_specs=(P("ka", None, None, "ga"), P(None, None, "ga"), P("ka")),
        out_specs=P("ga", "ka", None, None, None),
        check_vma=False,
    )
```

```python
import functools

import jax
import jax.numpy as jnp
from jax import lax
from jax.experimental import pallas as pl
from jax.experimental.pallas import tpu as pltpu
from jax.sharding import PartitionSpec as P

MESH = pl.DeviceIdType.MESH
BLOCK = 8
BAND_BLOCK = 32
UNROLL = 24
PSI = (False, False)
STAGE = (False, False)
PHI = (False, False)


def slab_at(ga, gn, step):
    if step == 0:
        return ga
    below, above = ga, gn - 1 - ga
    both = jnp.minimum(below, above)
    near = ga + (step + 1) // 2 if step % 2 else ga - step // 2
    far = jnp.where(above > below, ga + (step - both), ga - (step - both))
    return jnp.where(step <= 2 * both, near, far)


def pairs_of(gn):
    last = gn - 1
    halves = [(0, 0), (0, 1)] + [(s, side) for side in (1, 0) for s in range(1, last)] + [(last, 1), (last, 0)]
    return [halves[2 * c:2 * c + 2] for c in range(gn)]


def exchange(
    kn, gn, psi_hbm, dv_hbm, kq_ref, partial, tail_prods, phi_near, phi_wide,
    dv_ref, psi_near, psi_wide, dv_all, dv_f32, kq_all,
    stage_near, stage_wide, choice_near, choice_wide, table, prods,
    load, send_kq, send_one, send_own, send_slab, send_dv, send_psi, send_phi, send_stage,
    recv_kq, recv_one, recv_own, recv_slab, recv_dv, recv_psi, recv_phi, recv_stage,
):
    ka = lax.axis_index("ka")
    ga = lax.axis_index("ga")
    rows, half = stage_near.shape[1], stage_near.shape[2]
    bands = kn * rows // 2
    modes = partial.shape[0]
    others = pl.ds(0, kn - 1)

    def along_k(d):
        return lax.rem(ka + d, kn)

    def along_g(d):
        return lax.rem(ga + d, gn)

    first_half, second_half = pl.ds(0, half), pl.ds(half, half)
    loads = [
        pltpu.make_async_copy(psi_hbm.at[:, :, second_half], psi_wide.at[ga], load.at[0]),
        pltpu.make_async_copy(psi_hbm.at[:, :, first_half], psi_near.at[ga], load.at[1]),
        pltpu.make_async_copy(psi_hbm.at[ka, :, first_half], stage_near.at[ka], load.at[2]),
        pltpu.make_async_copy(psi_hbm.at[ka, :, second_half], stage_wide.at[ga, ka], load.at[3]),
        pltpu.make_async_copy(dv_hbm, dv_ref, load.at[4]),
    ]
    for c in loads:
        c.start()
    barrier = pltpu.get_barrier_semaphore()
    for d in range(1, gn):
        pl.semaphore_signal(barrier, inc=1, device_id=(ka, along_g(d)), device_id_type=MESH)
    for d in range(1, kn):
        pl.semaphore_signal(barrier, inc=1, device_id=(along_k(d), ga), device_id_type=MESH)
    for c in loads:
        c.wait()
    kq_all[ka] = kq_ref[...]
    pl.semaphore_wait(barrier, kn + gn - 2)

    def copy(src, dst, send, recv, to):
        return pltpu.make_async_remote_copy(
            src_ref=src, dst_ref=dst, send_sem=send, recv_sem=recv, device_id=to, device_id_type=MESH
        )

    def await_recv(ref, sem):
        copy(ref, ref, load.at[0], sem, (ka, ga)).wait_recv()

    def await_send(ref, sem):
        copy(ref, ref, sem, load.at[0], (ka, ga)).wait_send()

    def kq_start(d):
        copy(kq_ref, kq_all.at[ka], send_kq.at[0], recv_kq.at[0], (along_k(d), ga)).start()

    def one_start(side, d):
        to = along_k(d)
        if side:
            copy(psi_wide.at[ga, to], stage_wide.at[ga, ka], send_one.at[1], recv_one.at[1], (to, ga)).start()
        else:
            copy(psi_near.at[ga, to], stage_near.at[ka], send_one.at[0], recv_one.at[0], (to, ga)).start()

    def own_start(side, d):
        to = along_k(d)
        if side:
            copy(choice_wide.at[ga, to], phi_wide.at[ga, ka], send_own.at[1], recv_own.at[1], (to, ga)).start()
        else:
            copy(choice_near.at[to], phi_near.at[ga, ka], send_own.at[0], recv_own.at[0], (to, ga)).start()

    def slab_start(slab, d):
        to = along_k(d)
        copy(stage_wide.at[slab, to], psi_wide.at[slab, ka], send_slab.at[0], recv_slab.at[0, slab], (to, ga)).start()
        copy(choice_wide.at[slab, to], phi_wide.at[slab, ka], send_slab.at[1], recv_slab.at[1, slab], (to, ga)).start()

    shares, share = dv_all.shape[0], dv_all.shape[2]
    own_share = ka if shares > 1 else 0

    def dv_start(d):
        piece = dv_ref.at[along_g(d), pl.ds(own_share * share, share)]
        copy(piece, dv_all.at[own_share, ga], send_dv.at[0], recv_dv.at[0], (ka, along_g(d))).start()

    def dv_share_start(d):
        copy(dv_all.at[ka], dv_all.at[ka], send_dv.at[1], recv_dv.at[1], (along_k(d), ga)).start()

    def slab_copy(all_ref, send, recv, slab, to):
        return copy(all_ref.at[slab], all_ref.at[slab], send.at[to], recv.at[slab], (ka, to))

    def spread(slabs, act):
        hops = range(1, gn) if slabs.direct else range(1, max(gn - 1, 2))
        for hop in reversed(hops) if slabs.far_first else hops:
            for to in (ga + hop, ga - hop):
                @pl.when((to >= 0) & (to < gn))
                def _():
                    act(slabs, ga, to)

    def forward(slabs, act):
        copies = functools.partial(act, slabs)
        if gn > 2 and not slabs.direct:
            @pl.when(ga == 1)
            def _():
                copies(gn - 1, 0)

            @pl.when(ga == gn - 2)
            def _():
                copies(0, gn - 1)

    def is_far(slab):
        if gn <= 2:
            return ga < 0
        return ((ga == 1) & (slab == gn - 1)) | ((ga == gn - 2) & (slab == 0))

    psi_slab = functools.partial(slab_copy, psi_near, send_psi, recv_psi)
    phi_slab = functools.partial(slab_copy, phi_near, send_phi, recv_phi)
    stage_slab = functools.partial(slab_copy, stage_wide, send_stage, recv_stage)
    psi_slab.direct, psi_slab.far_first = PSI
    phi_slab.direct, phi_slab.far_first = PHI
    stage_slab.direct, stage_slab.far_first = STAGE

    def start(slabs, slab, to):
        slabs(slab, to).start()

    def finish_send(slabs, slab, to):
        slabs(slab, to).wait_send()

    def pass_on(slabs, far, to):
        slabs(far, ga).wait_recv()
        slabs(far, to).start()

    def await_slab(slabs, slab):
        if slabs.direct:
            slabs(slab, ga).wait_recv()
        else:
            @pl.when(jnp.logical_not(is_far(slab)))
            def _():
                slabs(slab, ga).wait_recv()

    wanted = []

    def choose(pieces, picks):
        table[...] = pieces[...]
        for k in range(kn):
            picks[k] = table[wanted[k]]

    spots = {half_slab: (c, i) for c, pair in enumerate(pairs_of(gn)) for i, half_slab in enumerate(pair)}

    def products(place, side):
        slab = slab_at(ga, gn, place)
        waves = psi_wide if side else psi_near
        lanes = slice(side * half, (side + 1) * half)
        chunk, start = spots[place, side]
        into = slice(start * half, (start + 1) * half)
        target = tail_prods if chunk == gn - 1 else prods.at[chunk]

        wave = waves.at[slab]
        span = min(BAND_BLOCK, rows)
        for first in range(0, bands, span):
            wave_real = wave[first // rows, first % rows:first % rows + span].astype(jnp.float32)
            low = bands + first
            wave_imag = wave[low // rows, low % rows:low % rows + span].astype(jnp.float32)

            def step(u, _):
                dv = dv_f32[slab, u]
                dv_real, dv_imag = dv[0:1, lanes], dv[1:2, lanes]
                target[u, first:first + span, into] = (dv_real * wave_real - dv_imag * wave_imag).astype(jnp.bfloat16)
                target[u, low:low + span, into] = (dv_real * wave_imag + dv_imag * wave_real).astype(jnp.bfloat16)
                return 0

            lax.fori_loop(0, modes, step, 0, unroll=UNROLL)

    def widen(slab):
        for i in range(shares):
            dv_f32[slab, i * share:(i + 1) * share] = dv_all[i, slab].astype(jnp.float32)

    block = BLOCK if modes % BLOCK == 0 else 1

    def block_products(place, side, first_mode):
        slab = slab_at(ga, gn, place)
        wave = (psi_wide if side else psi_near).at[slab]
        lanes = slice(side * half, (side + 1) * half)
        chunk, start = spots[place, side]
        into = slice(start * half, (start + 1) * half)
        span = min(BAND_BLOCK, rows)
        for first in range(0, bands, span):
            low = bands + first
            wave_real = wave[first // rows, first % rows:first % rows + span].astype(jnp.float32)
            wave_imag = wave[low // rows, low % rows:low % rows + span].astype(jnp.float32)
            for q in range(block):
                dv = dv_f32[slab, first_mode + q]
                dv_real, dv_imag = dv[0:1, lanes], dv[1:2, lanes]
                u = first_mode + q
                real = (dv_real * wave_real - dv_imag * wave_imag).astype(jnp.bfloat16)
                imag = (dv_real * wave_imag + dv_imag * wave_real).astype(jnp.bfloat16)
                prods[chunk, u, first:first + span, into] = real
                prods[chunk, u, low:low + span, into] = imag

    def matmul(chunk, fresh=()):
        sides = [(phi_wide if side else phi_near, slab_at(ga, gn, place)) for place, side in pairs_of(gn)[chunk]]

        def mode_step(t, _):
            for place, side in fresh:
                block_products(place, side, t * block)
            other = jnp.concatenate([ref[slab].reshape(2 * bands, half) for ref, slab in sides], axis=1)
            full = lax.dot_general(
                prods[chunk, pl.ds(t * block, block)].reshape(block * 2 * bands, 2 * half),
                other, (((1,), (1,)), ((), ())), preferred_element_type=jnp.float32,
            )
            for q in range(block):
                u = t * block + q
                top, low = full[2 * q * bands:(2 * q + 1) * bands], full[(2 * q + 1) * bands:(2 * q + 2) * bands]
                real = top[:, :bands] + low[:, bands:]
                imag = low[:, :bands] - top[:, bands:]
                if chunk:
                    real = real + partial[u, 0]
                    imag = imag + partial[u, 1]
                partial[u, 0] = real
                partial[u, 1] = imag
            return 0

        lax.fori_loop(0, modes // block, mode_step, 0, unroll=True)

    for d in range(1, kn):
        kq_start(d)
        one_start(1, d)
    for d in range(1, gn):
        dv_start(d)
    for d in range(1, kn):
        one_start(0, d)
    spread(psi_slab, start)
    dv_f32[ga] = dv_ref[ga].astype(jnp.float32)
    products(0, 0)
    products(0, 1)
    await_recv(kq_all.at[others], recv_kq.at[0])
    for k in range(kn):
        wanted.append(jnp.max(kq_all[k]))
    await_recv(stage_wide.at[ga, others], recv_one.at[1])
    spread(stage_slab, start)
    await_recv(stage_near.at[others], recv_one.at[0])
    choose(stage_near, choice_near)
    for d in range(1, kn):
        own_start(0, d)
    await_recv(dv_all.at[0, pl.ds(0, gn - 1)], recv_dv.at[0])
    if shares > 1:
        for d in range(1, kn):
            dv_share_start(d)
    choose(stage_wide.at[ga], choice_wide.at[ga])
    for d in range(1, kn):
        own_start(1, d)
    phi_near[ga, ka] = choice_near[ka]
    phi_wide[ga, ka] = choice_wide[ga, ka]
    forward(psi_slab, pass_on)
    await_recv(phi_near.at[ga, others], recv_own.at[0])
    spread(phi_slab, start)
    if shares > 1:
        await_recv(dv_all.at[others], recv_dv.at[1])

    def relay_step(step):
        slab = slab_at(ga, gn, step)
        await_slab(stage_slab, slab)
        choose(stage_wide.at[slab], choice_wide.at[slab])
        for d in range(1, kn):
            slab_start(slab, d)
        psi_wide[slab, ka] = stage_wide[slab, ka]
        phi_wide[slab, ka] = choice_wide[slab, ka]

    def near_step(step):
        slab = slab_at(ga, gn, step)
        widen(slab)
        await_slab(psi_slab, slab)
        products(step, 0)

    forward(stage_slab, pass_on)
    await_recv(phi_wide.at[ga, others], recv_own.at[1])
    for step in range(1, gn):
        relay_step(step)
        if step == 1:
            matmul(0)
        if step < gn - 1:
            near_step(step)
    forward(phi_slab, pass_on)
    near_step(gn - 1)
    for chunk in range(1, gn):
        for place, side in pairs_of(gn)[chunk]:
            slab = slab_at(ga, gn, place)
            if side:
                await_recv(psi_wide.at[slab, others], recv_slab.at[0, slab])
                await_recv(phi_wide.at[slab, others], recv_slab.at[1, slab])
                if chunk == gn - 1:
                    products(place, 1)
            else:
                await_slab(phi_slab, slab)
        if chunk < gn - 1:
            matmul(chunk, [(place, side) for place, side in pairs_of(gn)[chunk] if side])

    await_send(kq_all.at[others], send_kq.at[0])
    for side in range(2):
        await_send(stage_near.at[others], send_one.at[side])
        await_send(stage_near.at[others], send_own.at[side])
        await_send(stage_wide.at[pl.ds(0, gn - 1), others], send_slab.at[side])
    await_send(dv_all.at[0, pl.ds(0, gn - 1)], send_dv.at[0])
    if shares > 1:
        await_send(dv_all.at[others], send_dv.at[1])
    for slabs in (psi_slab, phi_slab, stage_slab):
        spread(slabs, finish_send)
        forward(slabs, finish_send)


def finish(gn, partial, prods, phi_near, phi_wide, out_hbm, out, done):
    ga = lax.axis_index("ga")
    modes, _, bands, _ = partial.shape
    half = phi_near.shape[3]
    sides = [(phi_wide if side else phi_near, slab_at(ga, gn, place)) for place, side in pairs_of(gn)[gn - 1]]
    other = jnp.concatenate([ref[slab].reshape(2 * bands, half) for ref, slab in sides], axis=1)

    def mode_step(u, _):
        full = lax.dot_general(prods[u], other, (((1,), (1,)), ((), ())), preferred_element_type=jnp.float32)
        top, low = full[:bands], full[bands:]
        out[u, 0] = (partial[u, 0] + (top[:, :bands] + low[:, bands:])).T
        out[u, 1] = (partial[u, 1] + (low[:, :bands] - top[:, bands:])).T
        pltpu.make_async_copy(out.at[u], out_hbm.at[u], done).start()
        return 0

    lax.fori_loop(0, modes, mode_step, 0, unroll=24)
    pltpu.make_async_copy(out, out_hbm, done).wait()


def body(psi, dvscf, kq_map):
    kn, gn = lax.axis_size("ka"), lax.axis_size("ga")
    _, parts, bands, cells = psi.shape
    rows = parts * bands // kn
    half = cells // 2
    modes = dvscf.shape[0] // gn
    shares = kn if modes % kn == 0 else 1
    pieces = pltpu.with_memory_space_constraint(psi.reshape(kn, rows, cells), pltpu.HBM)
    potential = pltpu.with_memory_space_constraint(dvscf.reshape(gn, modes, 2, cells), pltpu.HBM)
    wanted = jnp.broadcast_to(kq_map[:, None], (1, half)).astype(jnp.int32)
    dma = pltpu.SemaphoreType.DMA
    bf16 = jnp.bfloat16
    in_hbm, in_vmem = pl.BlockSpec(memory_space=pltpu.HBM), pl.BlockSpec(memory_space=pltpu.VMEM)
    partial, prods, phi_near, phi_wide = pl.pallas_call(
        functools.partial(exchange, kn, gn),
        out_shape=[
            jax.ShapeDtypeStruct((modes, 2, bands, bands), jnp.float32),
            jax.ShapeDtypeStruct((modes, 2 * bands, cells), bf16),
            jax.ShapeDtypeStruct((gn, kn, rows, half), bf16),
            jax.ShapeDtypeStruct((gn, kn, rows, half), bf16),
        ],
        in_specs=[in_hbm, in_hbm, in_vmem],
        out_specs=[in_vmem] * 4,
        scratch_shapes=[
            pltpu.VMEM((gn, modes, 2, cells), bf16),
            pltpu.VMEM((gn, kn, rows, half), bf16),
            pltpu.VMEM((gn, kn, rows, half), bf16),
            pltpu.VMEM((shares, gn, modes // shares, 2, cells), bf16),
            pltpu.VMEM((gn, modes, 2, cells), jnp.float32),
            pltpu.VMEM((kn, 1, half), jnp.int32),
            pltpu.VMEM((kn, rows, half), bf16),
            pltpu.VMEM((gn, kn, rows, half), bf16),
            pltpu.VMEM((kn, rows, half), bf16),
            pltpu.VMEM((gn, kn, rows, half), bf16),
            pltpu.VMEM((kn, rows, half), bf16),
            pltpu.VMEM((gn - 1, modes, 2 * bands, cells), bf16),
            dma((5,)),
            dma((1,)), dma((2,)), dma((2,)), dma((2,)), dma((2,)), dma((gn,)), dma((gn,)), dma((gn,)),
            dma((1,)), dma((2,)), dma((2,)), dma((2, gn)), dma((2,)), dma((gn,)), dma((gn,)), dma((gn,)),
        ],
        compiler_params=pltpu.CompilerParams(collective_id=0, has_side_effects=True, vmem_limit_bytes=40 * 1024 * 1024),
    )(pieces, potential, wanted)
    out = pl.pallas_call(
        functools.partial(finish, gn),
        out_shape=jax.ShapeDtypeStruct((modes, 2, bands, bands), jnp.float32),
        in_specs=[in_vmem] * 4,
        out_specs=in_hbm,
        scratch_shapes=[pltpu.VMEM((modes, 2, bands, bands), jnp.float32), dma],
        compiler_params=pltpu.CompilerParams(vmem_limit_bytes=16 * 1024 * 1024),
    )(partial, prods, phi_near, phi_wide)
    return out[:, None]


def solution(mesh):
    return jax.shard_map(
        body,
        mesh=mesh,
        in_specs=(P("ka", None, None, "ga"), P(None, None, "ga"), P("ka")),
        out_specs=P("ga", "ka", None, None, None),
        check_vma=False,
    )
```

```python
import functools

import jax
import jax.numpy as jnp
from jax import lax
from jax.experimental import pallas as pl
from jax.experimental.pallas import tpu as pltpu
from jax.sharding import PartitionSpec as P

MESH = pl.DeviceIdType.MESH
BLOCK = 8
BAND_BLOCK = 32
UNROLL = 24
PSI = (False, True)
STAGE = (False, True)
PHI = (False, False)


def slab_at(ga, gn, step):
    if step == 0:
        return ga
    below, above = ga, gn - 1 - ga
    both = jnp.minimum(below, above)
    near = ga + (step + 1) // 2 if step % 2 else ga - step // 2
    far = jnp.where(above > below, ga + (step - both), ga - (step - both))
    return jnp.where(step <= 2 * both, near, far)


def pairs_of(gn):
    last = gn - 1
    halves = [(0, 0), (0, 1)] + [(s, side) for side in (1, 0) for s in range(1, last)] + [(last, 1), (last, 0)]
    return [halves[2 * c:2 * c + 2] for c in range(gn)]


def exchange(
    kn, gn, psi_hbm, dv_hbm, kq_ref, partial, tail_prods, phi_near, phi_wide,
    dv_ref, psi_near, psi_wide, dv_all, dv_f32, kq_all,
    stage_near, stage_wide, choice_near, choice_wide, table, prods,
    load, send_kq, send_one, send_own, send_slab, send_dv, send_psi, send_phi, send_stage,
    recv_kq, recv_one, recv_own, recv_slab, recv_dv, recv_psi, recv_phi, recv_stage,
):
    ka = lax.axis_index("ka")
    ga = lax.axis_index("ga")
    rows, half = stage_near.shape[1], stage_near.shape[2]
    bands = kn * rows // 2
    modes = partial.shape[0]
    others = pl.ds(0, kn - 1)

    def along_k(d):
        return lax.rem(ka + d, kn)

    def along_g(d):
        return lax.rem(ga + d, gn)

    first_half, second_half = pl.ds(0, half), pl.ds(half, half)
    loads = [
        pltpu.make_async_copy(psi_hbm.at[:, :, second_half], psi_wide.at[ga], load.at[0]),
        pltpu.make_async_copy(psi_hbm.at[:, :, first_half], psi_near.at[ga], load.at[1]),
        pltpu.make_async_copy(psi_hbm.at[ka, :, first_half], stage_near.at[ka], load.at[2]),
        pltpu.make_async_copy(psi_hbm.at[ka, :, second_half], stage_wide.at[ga, ka], load.at[3]),
        pltpu.make_async_copy(dv_hbm, dv_ref, load.at[4]),
    ]
    for c in loads:
        c.start()
    barrier = pltpu.get_barrier_semaphore()
    for d in range(1, gn):
        pl.semaphore_signal(barrier, inc=1, device_id=(ka, along_g(d)), device_id_type=MESH)
    for d in range(1, kn):
        pl.semaphore_signal(barrier, inc=1, device_id=(along_k(d), ga), device_id_type=MESH)
    for c in loads:
        c.wait()
    kq_all[ka] = kq_ref[...]
    pl.semaphore_wait(barrier, kn + gn - 2)

    def copy(src, dst, send, recv, to):
        return pltpu.make_async_remote_copy(
            src_ref=src, dst_ref=dst, send_sem=send, recv_sem=recv, device_id=to, device_id_type=MESH
        )

    def await_recv(ref, sem):
        copy(ref, ref, load.at[0], sem, (ka, ga)).wait_recv()

    def await_send(ref, sem):
        copy(ref, ref, sem, load.at[0], (ka, ga)).wait_send()

    def kq_start(d):
        copy(kq_ref, kq_all.at[ka], send_kq.at[0], recv_kq.at[0], (along_k(d), ga)).start()

    def one_start(side, d):
        to = along_k(d)
        if side:
            copy(psi_wide.at[ga, to], stage_wide.at[ga, ka], send_one.at[1], recv_one.at[1], (to, ga)).start()
        else:
            copy(psi_near.at[ga, to], stage_near.at[ka], send_one.at[0], recv_one.at[0], (to, ga)).start()

    def own_start(side, d):
        to = along_k(d)
        if side:
            copy(choice_wide.at[ga, to], phi_wide.at[ga, ka], send_own.at[1], recv_own.at[1], (to, ga)).start()
        else:
            copy(choice_near.at[to], phi_near.at[ga, ka], send_own.at[0], recv_own.at[0], (to, ga)).start()

    def slab_start(slab, d):
        to = along_k(d)
        copy(stage_wide.at[slab, to], psi_wide.at[slab, ka], send_slab.at[0], recv_slab.at[0, slab], (to, ga)).start()
        copy(choice_wide.at[slab, to], phi_wide.at[slab, ka], send_slab.at[1], recv_slab.at[1, slab], (to, ga)).start()

    shares, share = dv_all.shape[0], dv_all.shape[2]
    own_share = ka if shares > 1 else 0

    def dv_start(d):
        piece = dv_ref.at[along_g(d), pl.ds(own_share * share, share)]
        copy(piece, dv_all.at[own_share, ga], send_dv.at[0], recv_dv.at[0], (ka, along_g(d))).start()

    def dv_share_start(d):
        copy(dv_all.at[ka], dv_all.at[ka], send_dv.at[1], recv_dv.at[1], (along_k(d), ga)).start()

    def slab_copy(all_ref, send, recv, slab, to):
        return copy(all_ref.at[slab], all_ref.at[slab], send.at[to], recv.at[slab], (ka, to))

    def spread(slabs, act):
        hops = range(1, gn) if slabs.direct else range(1, max(gn - 1, 2))
        for hop in reversed(hops) if slabs.far_first else hops:
            for to in (ga + hop, ga - hop):
                @pl.when((to >= 0) & (to < gn))
                def _():
                    act(slabs, ga, to)

    def forward(slabs, act):
        copies = functools.partial(act, slabs)
        if gn > 2 and not slabs.direct:
            @pl.when(ga == 1)
            def _():
                copies(gn - 1, 0)

            @pl.when(ga == gn - 2)
            def _():
                copies(0, gn - 1)

    def is_far(slab):
        if gn <= 2:
            return ga < 0
        return ((ga == 1) & (slab == gn - 1)) | ((ga == gn - 2) & (slab == 0))

    psi_slab = functools.partial(slab_copy, psi_near, send_psi, recv_psi)
    phi_slab = functools.partial(slab_copy, phi_near, send_phi, recv_phi)
    stage_slab = functools.partial(slab_copy, stage_wide, send_stage, recv_stage)
    psi_slab.direct, psi_slab.far_first = PSI
    phi_slab.direct, phi_slab.far_first = PHI
    stage_slab.direct, stage_slab.far_first = STAGE

    def start(slabs, slab, to):
        slabs(slab, to).start()

    def finish_send(slabs, slab, to):
        slabs(slab, to).wait_send()

    def pass_on(slabs, far, to):
        slabs(far, ga).wait_recv()
        slabs(far, to).start()

    def await_slab(slabs, slab):
        if slabs.direct:
            slabs(slab, ga).wait_recv()
        else:
            @pl.when(jnp.logical_not(is_far(slab)))
            def _():
                slabs(slab, ga).wait_recv()

    wanted = []

    def choose(pieces, picks):
        table[...] = pieces[...]
        for k in range(kn):
            picks[k] = table[wanted[k]]

    spots = {half_slab: (c, i) for c, pair in enumerate(pairs_of(gn)) for i, half_slab in enumerate(pair)}

    def products(place, side):
        slab = slab_at(ga, gn, place)
        waves = psi_wide if side else psi_near
        lanes = slice(side * half, (side + 1) * half)
        chunk, start = spots[place, side]
        into = slice(start * half, (start + 1) * half)
        target = tail_prods if chunk == gn - 1 else prods.at[chunk]

        wave = waves.at[slab]
        span = min(BAND_BLOCK, rows)
        for first in range(0, bands, span):
            wave_real = wave[first // rows, first % rows:first % rows + span].astype(jnp.float32)
            low = bands + first
            wave_imag = wave[low // rows, low % rows:low % rows + span].astype(jnp.float32)

            def step(u, _):
                dv = dv_f32[slab, u]
                dv_real, dv_imag = dv[0:1, lanes], dv[1:2, lanes]
                target[u, first:first + span, into] = (dv_real * wave_real - dv_imag * wave_imag).astype(jnp.bfloat16)
                target[u, low:low + span, into] = (dv_real * wave_imag + dv_imag * wave_real).astype(jnp.bfloat16)
                return 0

            lax.fori_loop(0, modes, step, 0, unroll=UNROLL)

    def widen(slab):
        for i in range(shares):
            dv_f32[slab, i * share:(i + 1) * share] = dv_all[i, slab].astype(jnp.float32)

    block = BLOCK if modes % BLOCK == 0 else 1

    def block_products(place, side, first_mode):
        slab = slab_at(ga, gn, place)
        wave = (psi_wide if side else psi_near).at[slab]
        lanes = slice(side * half, (side + 1) * half)
        chunk, start = spots[place, side]
        into = slice(start * half, (start + 1) * half)
        span = min(BAND_BLOCK, rows)
        for first in range(0, bands, span):
            low = bands + first
            wave_real = wave[first // rows, first % rows:first % rows + span].astype(jnp.float32)
            wave_imag = wave[low // rows, low % rows:low % rows + span].astype(jnp.float32)
            for q in range(block):
                dv = dv_f32[slab, first_mode + q]
                dv_real, dv_imag = dv[0:1, lanes], dv[1:2, lanes]
                u = first_mode + q
                real = (dv_real * wave_real - dv_imag * wave_imag).astype(jnp.bfloat16)
                imag = (dv_real * wave_imag + dv_imag * wave_real).astype(jnp.bfloat16)
                prods[chunk, u, first:first + span, into] = real
                prods[chunk, u, low:low + span, into] = imag

    def matmul(chunk, fresh=()):
        sides = [(phi_wide if side else phi_near, slab_at(ga, gn, place)) for place, side in pairs_of(gn)[chunk]]

        def mode_step(t, _):
            for place, side in fresh:
                block_products(place, side, t * block)
            other = jnp.concatenate([ref[slab].reshape(2 * bands, half) for ref, slab in sides], axis=1)
            full = lax.dot_general(
                prods[chunk, pl.ds(t * block, block)].reshape(block * 2 * bands, 2 * half),
                other, (((1,), (1,)), ((), ())), preferred_element_type=jnp.float32,
            )
            for q in range(block):
                u = t * block + q
                top, low = full[2 * q * bands:(2 * q + 1) * bands], full[(2 * q + 1) * bands:(2 * q + 2) * bands]
                real = top[:, :bands] + low[:, bands:]
                imag = low[:, :bands] - top[:, bands:]
                if chunk:
                    real = real + partial[u, 0]
                    imag = imag + partial[u, 1]
                partial[u, 0] = real
                partial[u, 1] = imag
            return 0

        lax.fori_loop(0, modes // block, mode_step, 0, unroll=True)

    for d in range(1, kn):
        kq_start(d)
        one_start(1, d)
    for d in range(1, gn):
        dv_start(d)
    for d in range(1, kn):
        one_start(0, d)
    spread(psi_slab, start)
    dv_f32[ga] = dv_ref[ga].astype(jnp.float32)
    products(0, 0)
    products(0, 1)
    await_recv(kq_all.at[others], recv_kq.at[0])
    for k in range(kn):
        wanted.append(jnp.max(kq_all[k]))
    await_recv(stage_wide.at[ga, others], recv_one.at[1])
    spread(stage_slab, start)
    await_recv(stage_near.at[others], recv_one.at[0])
    choose(stage_near, choice_near)
    for d in range(1, kn):
        own_start(0, d)
    await_recv(dv_all.at[0, pl.ds(0, gn - 1)], recv_dv.at[0])
    if shares > 1:
        for d in range(1, kn):
            dv_share_start(d)
    choose(stage_wide.at[ga], choice_wide.at[ga])
    for d in range(1, kn):
        own_start(1, d)
    phi_near[ga, ka] = choice_near[ka]
    phi_wide[ga, ka] = choice_wide[ga, ka]
    forward(psi_slab, pass_on)
    await_recv(phi_near.at[ga, others], recv_own.at[0])
    spread(phi_slab, start)
    if shares > 1:
        await_recv(dv_all.at[others], recv_dv.at[1])

    def relay_step(step):
        slab = slab_at(ga, gn, step)
        await_slab(stage_slab, slab)
        choose(stage_wide.at[slab], choice_wide.at[slab])
        for d in range(1, kn):
            slab_start(slab, d)
        psi_wide[slab, ka] = stage_wide[slab, ka]
        phi_wide[slab, ka] = choice_wide[slab, ka]

    def near_step(step):
        slab = slab_at(ga, gn, step)
        widen(slab)
        await_slab(psi_slab, slab)
        products(step, 0)

    forward(stage_slab, pass_on)
    await_recv(phi_wide.at[ga, others], recv_own.at[1])
    for step in range(1, gn):
        relay_step(step)
        if step == 1:
            matmul(0)
        if step < gn - 1:
            near_step(step)
    forward(phi_slab, pass_on)
    near_step(gn - 1)
    for chunk in range(1, gn):
        for place, side in pairs_of(gn)[chunk]:
            slab = slab_at(ga, gn, place)
            if side:
                await_recv(psi_wide.at[slab, others], recv_slab.at[0, slab])
                await_recv(phi_wide.at[slab, others], recv_slab.at[1, slab])
                if chunk == gn - 1:
                    products(place, 1)
            else:
                await_slab(phi_slab, slab)
        if chunk < gn - 1:
            matmul(chunk, [(place, side) for place, side in pairs_of(gn)[chunk] if side])

    await_send(kq_all.at[others], send_kq.at[0])
    for side in range(2):
        await_send(stage_near.at[others], send_one.at[side])
        await_send(stage_near.at[others], send_own.at[side])
        await_send(stage_wide.at[pl.ds(0, gn - 1), others], send_slab.at[side])
    await_send(dv_all.at[0, pl.ds(0, gn - 1)], send_dv.at[0])
    if shares > 1:
        await_send(dv_all.at[others], send_dv.at[1])
    for slabs in (psi_slab, phi_slab, stage_slab):
        spread(slabs, finish_send)
        forward(slabs, finish_send)


def finish(gn, partial, prods, phi_near, phi_wide, out_hbm, out, done):
    ga = lax.axis_index("ga")
    modes, _, bands, _ = partial.shape
    half = phi_near.shape[3]
    sides = [(phi_wide if side else phi_near, slab_at(ga, gn, place)) for place, side in pairs_of(gn)[gn - 1]]
    other = jnp.concatenate([ref[slab].reshape(2 * bands, half) for ref, slab in sides], axis=1)

    def mode_step(u, _):
        full = lax.dot_general(prods[u], other, (((1,), (1,)), ((), ())), preferred_element_type=jnp.float32)
        top, low = full[:bands], full[bands:]
        out[u, 0] = (partial[u, 0] + (top[:, :bands] + low[:, bands:])).T
        out[u, 1] = (partial[u, 1] + (low[:, :bands] - top[:, bands:])).T
        pltpu.make_async_copy(out.at[u], out_hbm.at[u], done).start()
        return 0

    lax.fori_loop(0, modes, mode_step, 0, unroll=24)
    pltpu.make_async_copy(out, out_hbm, done).wait()


def body(psi, dvscf, kq_map):
    kn, gn = lax.axis_size("ka"), lax.axis_size("ga")
    _, parts, bands, cells = psi.shape
    rows = parts * bands // kn
    half = cells // 2
    modes = dvscf.shape[0] // gn
    shares = kn if modes % kn == 0 else 1
    pieces = pltpu.with_memory_space_constraint(psi.reshape(kn, rows, cells), pltpu.HBM)
    potential = pltpu.with_memory_space_constraint(dvscf.reshape(gn, modes, 2, cells), pltpu.HBM)
    wanted = jnp.broadcast_to(kq_map[:, None], (1, half)).astype(jnp.int32)
    dma = pltpu.SemaphoreType.DMA
    bf16 = jnp.bfloat16
    in_hbm, in_vmem = pl.BlockSpec(memory_space=pltpu.HBM), pl.BlockSpec(memory_space=pltpu.VMEM)
    partial, prods, phi_near, phi_wide = pl.pallas_call(
        functools.partial(exchange, kn, gn),
        out_shape=[
            jax.ShapeDtypeStruct((modes, 2, bands, bands), jnp.float32),
            jax.ShapeDtypeStruct((modes, 2 * bands, cells), bf16),
            jax.ShapeDtypeStruct((gn, kn, rows, half), bf16),
            jax.ShapeDtypeStruct((gn, kn, rows, half), bf16),
        ],
        in_specs=[in_hbm, in_hbm, in_vmem],
        out_specs=[in_vmem] * 4,
        scratch_shapes=[
            pltpu.VMEM((gn, modes, 2, cells), bf16),
            pltpu.VMEM((gn, kn, rows, half), bf16),
            pltpu.VMEM((gn, kn, rows, half), bf16),
            pltpu.VMEM((shares, gn, modes // shares, 2, cells), bf16),
            pltpu.VMEM((gn, modes, 2, cells), jnp.float32),
            pltpu.VMEM((kn, 1, half), jnp.int32),
            pltpu.VMEM((kn, rows, half), bf16),
            pltpu.VMEM((gn, kn, rows, half), bf16),
            pltpu.VMEM((kn, rows, half), bf16),
            pltpu.VMEM((gn, kn, rows, half), bf16),
            pltpu.VMEM((kn, rows, half), bf16),
            pltpu.VMEM((gn - 1, modes, 2 * bands, cells), bf16),
            dma((5,)),
            dma((1,)), dma((2,)), dma((2,)), dma((2,)), dma((2,)), dma((gn,)), dma((gn,)), dma((gn,)),
            dma((1,)), dma((2,)), dma((2,)), dma((2, gn)), dma((2,)), dma((gn,)), dma((gn,)), dma((gn,)),
        ],
        compiler_params=pltpu.CompilerParams(collective_id=0, has_side_effects=True, vmem_limit_bytes=40 * 1024 * 1024),
    )(pieces, potential, wanted)
    out = pl.pallas_call(
        functools.partial(finish, gn),
        out_shape=jax.ShapeDtypeStruct((modes, 2, bands, bands), jnp.float32),
        in_specs=[in_vmem] * 4,
        out_specs=in_hbm,
        scratch_shapes=[pltpu.VMEM((modes, 2, bands, bands), jnp.float32), dma],
        compiler_params=pltpu.CompilerParams(vmem_limit_bytes=16 * 1024 * 1024),
    )(partial, prods, phi_near, phi_wide)
    return out[:, None]


def solution(mesh):
    return jax.shard_map(
        body,
        mesh=mesh,
        in_specs=(P("ka", None, None, "ga"), P(None, None, "ga"), P("ka")),
        out_specs=P("ga", "ka", None, None, None),
        check_vma=False,
    )
```
